256 devices in a mesh: row: 16 (over x_lo, z), col: 16 (over x_hi, y, core).
Axes of the slice: x: 4 (x_hi: 2, x_lo: 2; x = x_hi * 2 + x_lo), y: 4, z: 8, core: 2. Of those that a mesh axis runs over, the one named last changes fastest.
Arguments:
- forward_map: float32 [2048, 16384], P('row', 'col'), may hold values from -0.125 to 0.125
- sensor_weights: float32 [2048], P('row'), may hold values from 0.25 to 4
- sensor_mask: int32 [2048], P('row'), may hold values 0 or 1
Outputs:
- gram_matrix: float32 [16384, 16384], P('row', 'col')
The draws below stay inside these ranges and needn't reach their ends.
All inputs are finite; a program needn't handle non-finite values. No bound on the sum of `sensor_mask` on one device may be relied on, other than what follows from the above.
Results may differ from the reference program's by a relative error of at most 0.000061.
Values sent between devices are 32-bit elements; how exact they have to be, the bound alone decides.
A program may use at most 128 MiB of HBM per device.

```python
import math
import jax
import jax.numpy as jnp
from jax import lax

PARAMS = 16384
OBS = 2048


def with_ends(array, stream_key, least, largest):
    longest = array.shape.index(max(array.shape))
    spots = []
    for shift in (0, 1):
        where = [jax.random.randint(jax.random.fold_in(stream_key, axis), (), 0, length) for axis, length in enumerate(array.shape)]
        where[longest] = (where[longest] + shift) % array.shape[longest]
        spots.append(tuple(where))
    return array.at[spots[0]].set(least).at[spots[1]].set(largest)


def level_of(own_key, extent, shards, least, largest):
    level, own = 1.0, jax.random.fold_in(own_key, 6)
    for dim, shards_of in shards:
        steps = jnp.exp(jax.random.uniform(jax.random.fold_in(own, dim), (shards_of,), jnp.float32, least / len(shards), largest / len(shards)))
        level = level * jnp.repeat(steps, extent[dim] // shards_of).reshape([-1 if axis == dim else 1 for axis in range(len(extent))])
    return level


def centred(own_key, shape, width, most, pieces=(), held_as=jnp.bfloat16):
    gain = level_of(own_key, shape, pieces, -0.22, 0.18) if pieces else 1.0
    result = jax.random.normal(own_key, shape, jnp.float32) * width * gain
    return jnp.minimum(jnp.maximum(result, -most), most).astype(held_as)


def setup_inputs(seed: int = 0) -> dict:
    key_of = jax.random.split(jax.random.key(seed), 4)
    return {
        "forward_map": centred(key_of[0], (OBS, PARAMS), OBS ** -0.5, 0.125, ((0, 16), (1, 16)), jnp.float32),
        "sensor_weights": jnp.clip(jnp.exp(math.log(4.0) - 2.7725887 * jax.random.uniform(key_of[1], (OBS,), jnp.float32) ** level_of(key_of[1], (OBS,), ((0, 16),), -0.2, 0.2)), 0.25, 4.0),
        "sensor_mask": with_ends((jax.random.randint(key_of[2], (OBS,), 0, 2) < 1).astype(jnp.int32), jax.random.fold_in(key_of[2], 1), 0, 1),
    }


def reference(forward_map, sensor_weights, sensor_mask):
    sensor_scale = sensor_weights * sensor_mask.astype(jnp.float32)
    weighted = forward_map * sensor_scale[:, None]
    return lax.dot_general(forward_map, weighted, (((0,), (0,)), ((), ())), precision=lax.Precision.HIGHEST, preferred_element_type=jnp.float32)
```

```python
import functools

import jax
import jax.numpy as jnp
from jax import lax
from jax.experimental import pallas as pl
from jax.experimental.pallas import tpu as pltpu
from jax.sharding import PartitionSpec as P

MESH = pl.DeviceIdType.MESH
OBS, SIDE = 2048, 1024
PIECE, STEPS, CUTS = 16, 5, 8
SLOTS = STEPS * CUTS
TRIO = 3 * PIECE
LEFT = OBS

PARENT = ((0, 0, 0), (1, 2, 1), (4, 5, 5), (7, 3, 7), (6, 9, 10))

OUTER = (
    tuple((i, i) for i in range(0, 4)),
    tuple((i, i) for i in range(4, 10)),
    tuple((i, i) for i in range(10, 16)),
)
INNER = (
    ((0, 3), (3, 0), (1, 6), (6, 1)),
    ((5, 9), (9, 5), (7, 12), (12, 7), (2, 11), (11, 2)),
    ((4, 13), (13, 4), (8, 14), (14, 8), (10, 15), (15, 10)),
)
HOP = 3
LAG = 4 * HOP + 2
TURNS = SLOTS + LAG


def base_of(block):
    return 128 + CUTS * TRIO * ((block - 1) // 3) + PIECE * ((block - 1) % 3)


def row_of(block, cut):
    return PIECE * cut if block == 0 else base_of(block) + TRIO * cut


def pick(choice, values):
    out = values[-1]
    for i in reversed(range(len(values) - 1)):
        out = jnp.where(choice == i, values[i], out)
    return out


def kernel(
    map_ref, weights_ref, mask_ref, gram_ref,
    store, relay, scales, columns, right_hi, right_lo, left_hi, left_lo, total,
    load_sem, slot_sem, left_sem, left_own_sem, relay_sem, relay_own_sem, scale_sem,
    sent_sem, sent_scale_sem, plus_sem, minus_sem, twin_sem, cross_sem, toward_sem, onward_sem, out_sem,
):
    row, col = lax.axis_index("row"), lax.axis_index("col")
    x_lo, z = row // 8, row % 8
    x_hi, y, core = col // 8, (col // 2) % 4, col % 2
    up = (x_lo * 8 + (z + 1) % 8, col)
    down = (x_lo * 8 + (z + 7) % 8, col)
    pair = ((1 - x_lo) * 8 + z, col)
    plus = (row, x_hi * 8 + ((y + 1) % 4) * 2 + core)
    minus = (row, x_hi * 8 + ((y + 3) % 4) * 2 + core)
    twin = (row, x_hi * 8 + y * 2 + (1 - core))
    across = ((1 - x_lo) * 8 + z, (1 - x_hi) * 8 + y * 2 + core)
    links = (up, down, pair)
    outer = x_hi == x_lo
    inner = x_hi != x_lo
    first = core == z % 2
    dy = (y + 4 - z // 2) % 4

    def loading(cut):
        rows = pl.ds(PIECE * cut, PIECE)
        return pltpu.make_async_copy(map_ref.at[rows], store.at[rows], load_sem.at[cut])

    for cut in range(CUTS):
        loading(cut).start()
    scale = weights_ref[...] * mask_ref[...].astype(jnp.float32)
    scales[pl.ds(0, 8), :] = jnp.broadcast_to(scale, (8, 128))
    total[...] = jnp.zeros_like(total)

    barrier = pltpu.get_barrier_semaphore()
    for other in (up, down, pair, plus, minus, twin, across):
        pl.semaphore_signal(barrier, inc=1, device_id=other, device_id_type=MESH)
    pl.semaphore_wait(barrier, 7)

    def remote(source, target, sent, arrived, device):
        return pltpu.make_async_remote_copy(
            src_ref=source, dst_ref=target, send_sem=sent, recv_sem=arrived,
            device_id=device, device_id_type=MESH,
        )

    def arrival(ref, sem):
        return remote(ref, ref, sent_sem.at[0], sem, up)

    def span(start, size):
        return store.at[pl.ds(pl.multiple_of(start, 8), size)]

    def send_scale(source_block, step, g):
        remote(
            scales.at[pl.ds(8 * source_block, 8)],
            scales.at[pl.ds(pl.multiple_of(8 * (3 * step + 1 + g), 8), 8)],
            sent_scale_sem.at[0], scale_sem.at[step], links[g],
        ).start()

    for g in range(3):
        send_scale(0, 0, g)
    for cut in range(CUTS):
        loading(cut).wait()
        for g in range(3):
            remote(
                span(PIECE * cut, PIECE), span(128 + TRIO * cut + PIECE * g, PIECE),
                sent_sem.at[0], slot_sem.at[cut], links[g],
            ).start()

    def expand(block, start):
        square = jnp.broadcast_to(scales[pl.ds(pl.multiple_of(start, 8), 1), :], (128, 128))
        columns[block] = square.T

    back = (4 - dy) % 4
    hops = []
    for lane in range(4):
        on_outer = dy if lane % 2 == 0 else back
        on_inner = (1 + dy, 1 + back, pick(dy, (3, 2, 3, 4)), pick(dy, (3, 4, 3, 2)))[lane]
        hops.append(jnp.where(outer, on_outer, on_inner))
    goes_plus = (
        jnp.where(outer, dy <= 2, dy <= 2),
        inner & (dy < 0),
        jnp.where(outer, dy <= 2, (dy == 1) | (dy == 2)),
        inner & (dy == 3),
    )
    goes_minus = (
        inner & (dy < 0),
        jnp.where(outer, dy != 1, dy != 1),
        inner & (dy == 1),
        jnp.where(outer, dy != 1, (dy == 2) | (dy == 3)),
    )
    at_source = outer & (dy == 0) & first
    from_row = jnp.where(at_source, 0, LEFT)

    def pass_on(slot, source_row, device, sent):
        remote(
            span(source_row + 128 + TRIO * slot, TRIO), span(LEFT + 128 + TRIO * slot, TRIO),
            sent, left_sem.at[slot], device,
        ).start()

        @pl.when(slot < CUTS)
        def _():
            remote(
                span(source_row + PIECE * slot, PIECE), span(LEFT + PIECE * slot, PIECE),
                sent, left_own_sem.at[slot], device,
            ).start()

    def into_relay(slot, device, sent):
        fourth = slot // 4
        remote(
            span(128 + TRIO * slot, TRIO), relay.at[pl.ds(pl.multiple_of(TRIO * fourth, 8), TRIO)],
            sent, relay_sem.at[fourth], device,
        ).start()

        @pl.when(slot < CUTS)
        def _():
            remote(
                span(PIECE * slot, PIECE), relay.at[pl.ds(pl.multiple_of(480 + PIECE * fourth, 8), PIECE)],
                sent, relay_own_sem.at[fourth], device,
            ).start()

    def out_of_relay(slot):
        fourth = slot // 4
        held = relay.at[pl.ds(pl.multiple_of(TRIO * fourth, 8), TRIO)]
        arrival(held, relay_sem.at[fourth]).wait_recv()
        remote(held, span(LEFT + 128 + TRIO * slot, TRIO), onward_sem.at[0], left_sem.at[slot], across).start()

        @pl.when(slot < CUTS)
        def _():
            own = relay.at[pl.ds(pl.multiple_of(480 + PIECE * fourth, 8), PIECE)]
            arrival(own, relay_own_sem.at[fourth]).wait_recv()
            remote(own, span(LEFT + PIECE * slot, PIECE), onward_sem.at[0], left_own_sem.at[slot], across).start()

    def split(turn, start, phase, base, pieces):
        cut = turn - start

        @pl.when((turn >= start) & (turn < start + CUTS))
        def _():
            for n in range(pieces):
                (right_o, left_o), (right_i, left_i) = OUTER[phase][n], INNER[phase][n]

                def start_of(a, b):
                    def one(block):
                        return PIECE * cut if block == 0 else base_of(block) + TRIO * cut

                    return one(a) if a == b else jnp.where(outer, one(a), one(b))

                right_row = pl.multiple_of(start_of(right_o, right_i), 8)
                left_row = pl.multiple_of(LEFT + start_of(left_o, left_i), 8)
                block = right_o if right_o == right_i else jnp.where(outer, right_o, right_i)
                put = pl.ds(pl.multiple_of(base + PIECE * (pieces * cut + n), 16), PIECE)
                factor = columns[block, pl.ds(pl.multiple_of(PIECE * cut, 8), PIECE), :]
                for lane in range(SIDE // 128):
                    at = pl.ds(128 * lane, 128)
                    value = store[pl.ds(right_row, PIECE), at] * factor
                    high = value.astype(jnp.bfloat16)
                    right_hi[put, at] = high
                    right_lo[put, at] = (value - high.astype(jnp.float32)).astype(jnp.bfloat16)
                left_from = jnp.where(at_source, left_row - LEFT, left_row)
                value = store[pl.ds(pl.multiple_of(left_from, 8), PIECE), :]
                high = value.astype(jnp.bfloat16)
                left_hi[put, :] = high
                left_lo[put, :] = (value - high.astype(jnp.float32)).astype(jnp.bfloat16)

    def written(n):
        return pltpu.make_async_copy(total.at[n], gram_ref.at[:, pl.ds(256 * n, 256)], out_sem.at[n])

    def multiply(unit):
        k = pl.ds(pl.multiple_of(256 * unit, 256), 256)

        @pl.loop(0, 4)
        def _(n):
            at = pl.ds(pl.multiple_of(256 * n, 256), 256)

            def product(a, b):
                return lax.dot_general(
                    a[k, :], b[k, at], (((0,), (0,)), ((), ())), preferred_element_type=jnp.float32
                )

            total[n] += product(left_hi, right_hi) + product(left_hi, right_lo) + product(left_lo, right_hi)

            @pl.when(unit == 7)
            def _():
                written(n).start()

    @pl.loop(0, TURNS)
    def _(turn):
        step, cut, lane_now = turn // CUTS, turn % CUTS, turn % 4

        @pl.when(turn < SLOTS)
        def _():
            arrival(span(128 + TRIO * turn, TRIO), slot_sem.at[turn]).wait_recv()

            @pl.when(cut == 0)
            def _():
                arrival(scales.at[pl.ds(pl.multiple_of(8 + 24 * step, 8), 24)], scale_sem.at[step]).wait_recv()
                for g in range(3):
                    @pl.when(step < STEPS - 1)
                    def _():
                        source = pick(step, tuple(PARENT[s][g] for s in range(1, STEPS)))
                        remote(
                            scales.at[pl.ds(pl.multiple_of(8 * source, 8), 8)],
                            scales.at[pl.ds(pl.multiple_of(8 * (3 * step + 4 + g), 8), 8)],
                            sent_scale_sem.at[0], scale_sem.at[step + 1], links[g],
                        ).start()

            @pl.when(step < STEPS - 1)
            def _():
                for g in range(3):
                    base = pick(step, tuple(base_of(PARENT[s][g]) for s in range(1, STEPS)))
                    remote(
                        span(base + TRIO * cut, PIECE), span(128 + TRIO * (turn + CUTS) + PIECE * g, PIECE),
                        sent_sem.at[step + 1], slot_sem.at[turn + CUTS], links[g],
                    ).start()

            @pl.when(inner & first & (dy == 0))
            def _():
                @pl.when(lane_now < 2)
                def _():
                    pass_on(turn, 0, across, cross_sem.at[0])

                @pl.when(lane_now == 2)
                def _():
                    into_relay(turn, plus, toward_sem.at[0])

                @pl.when(lane_now == 3)
                def _():
                    into_relay(turn, minus, toward_sem.at[1])

        for lane, place in ((2, 1), (3, 3)):
            slot = turn - HOP

            @pl.when(inner & first & (dy == place) & (slot >= 0) & (slot < SLOTS) & ((slot + 4) % 4 == lane))
            def _():
                out_of_relay(slot)

        for lane in range(4):
            slot = turn - HOP * hops[lane] - jnp.where(first, 0, 1)

            @pl.when((slot >= 0) & (slot < SLOTS) & ((slot + 32) % 4 == lane))
            def _():
                @pl.when(jnp.logical_not(at_source))
                def _():
                    arrival(span(LEFT + 128 + TRIO * slot, TRIO), left_sem.at[slot]).wait_recv()

                    @pl.when(slot < CUTS)
                    def _():
                        arrival(span(LEFT + PIECE * slot, PIECE), left_own_sem.at[slot]).wait_recv()

                @pl.when(first & goes_plus[lane])
                def _():
                    pass_on(slot, from_row, plus, plus_sem.at[lane])

                @pl.when(first & goes_minus[lane])
                def _():
                    pass_on(slot, from_row, minus, minus_sem.at[lane])

                @pl.when(first)
                def _():
                    pass_on(slot, from_row, twin, twin_sem.at[lane])

        start_a, start_b, start_c = CUTS + LAG, 3 * CUTS + LAG, 4 * CUTS + LAG

        @pl.when(turn == start_a)
        def _():
            for block in range(10):
                expand(block, 8 * block)

        @pl.when(turn == start_c)
        def _():
            for block in range(10, 16):
                expand(block, 8 * block)

        @pl.when(turn == start_b)
        def _():
            for block in range(10, 13):
                expand(block, 8 * block)

        split(turn, start_a, 0, 0, 4)
        split(turn, start_b, 1, 512, 6)
        split(turn, start_c, 2, 1280, 6)
        in_a, in_b, in_c = turn - start_a, turn - start_b, turn - start_c
        due, unit = False, 0
        for at, number in (
            (start_a + 3, 0), (start_a + 7, 1),
            (start_b + 2, 2), (start_b + 5, 3), (start_b + 7, 4),
            (start_c + 2, 5), (start_c + 5, 6), (start_c + 7, 7),
        ):
            due = due | (turn == at)
            unit = jnp.where(turn == at, number, unit)

        @pl.when(due)
        def _():
            multiply(unit)

    for step in range(STEPS):
        remote(
            span(0, CUTS * TRIO), span(0, CUTS * TRIO), sent_sem.at[step], slot_sem.at[0], up
        ).wait_send()
    remote(
        scales.at[pl.ds(8, 120)], scales.at[pl.ds(8, 120)], sent_scale_sem.at[0], slot_sem.at[0], up
    ).wait_send()

    def drain(sem, rows):
        remote(span(0, rows), span(0, rows), sem, slot_sem.at[0], up).wait_send()

    for lane in range(4):
        @pl.when(first & goes_plus[lane])
        def _():
            drain(plus_sem.at[lane], 512)

        @pl.when(first & goes_minus[lane])
        def _():
            drain(minus_sem.at[lane], 512)

        @pl.when(first)
        def _():
            drain(twin_sem.at[lane], 512)

    @pl.when(inner & first & (dy == 0))
    def _():
        drain(cross_sem.at[0], 1024)
        drain(toward_sem.at[0], 512)
        drain(toward_sem.at[1], 512)

    @pl.when(inner & first & ((dy == 1) | (dy == 3)))
    def _():
        drain(onward_sem.at[0], 512)

    for n in range(4):
        written(n).wait()


def per_device(forward_map, sensor_weights, sensor_mask):
    dma = pltpu.SemaphoreType.DMA
    half = pltpu.VMEM((OBS, SIDE), jnp.bfloat16)
    return pl.pallas_call(
        kernel,
        out_shape=jax.ShapeDtypeStruct((SIDE, SIDE), jnp.float32),
        in_specs=[
            pl.BlockSpec(memory_space=pl.ANY),
            pl.BlockSpec(memory_space=pltpu.VMEM),
            pl.BlockSpec(memory_space=pltpu.VMEM),
        ],
        out_specs=pl.BlockSpec(memory_space=pl.ANY),
        scratch_shapes=[
            pltpu.VMEM((2 * OBS, SIDE), jnp.float32),
            pltpu.VMEM((512, SIDE), jnp.float32),
            pltpu.VMEM((128, 128), jnp.float32),
            pltpu.VMEM((16, 128, 128), jnp.float32),
            half, half, half, half,
            pltpu.VMEM((4, SIDE, 256), jnp.float32),
            dma((CUTS,)), dma((SLOTS,)), dma((SLOTS,)), dma((CUTS,)), dma((10,)), dma((2,)), dma((STEPS,)),
            dma((STEPS,)), dma((1,)), dma((4,)), dma((4,)), dma((4,)), dma((1,)), dma((2,)), dma((1,)), dma((4,)),
        ],
        compiler_params=pltpu.CompilerParams(
            collective_id=0, has_side_effects=True, vmem_limit_bytes=56 * 1024 * 1024
        ),
        cost_estimate=pl.CostEstimate(
            flops=2 * OBS * SIDE * SIDE, bytes_accessed=8 * SIDE * SIDE, transcendentals=0
        ),
    )(forward_map, sensor_weights.reshape(1, -1), sensor_mask.reshape(1, -1))


def solution(mesh):
    placed = (P("row", "col"), P("row"), P("row"))
    return jax.shard_map(
        per_device, mesh=mesh, in_specs=placed, out_specs=P("row", "col"), check_vma=False
    )
```

```python
import functools

import jax
import jax.numpy as jnp
from jax import lax
from jax.experimental import pallas as pl
from jax.experimental.pallas import tpu as pltpu
from jax.sharding import PartitionSpec as P

MESH = pl.DeviceIdType.MESH
OBS, SIDE = 2048, 1024
PIECE, STEPS, CUTS = 16, 5, 8
SLOTS = STEPS * CUTS
TRIO = 3 * PIECE
LEFT = OBS

PARENT = ((0, 0, 0), (1, 3, 1), (4, 2, 4), (7, 8, 8), (9, 12, 10))

OUTER = (
    tuple((i, i) for i in range(0, 4)),
    tuple((i, i) for i in range(4, 7)),
    tuple((i, i) for i in range(7, 10)),
    tuple((i, i) for i in range(10, 13)),
    tuple((i, i) for i in range(13, 16)),
)
INNER = (
    ((0, 3), (3, 0), (6, 1), (5, 2)),
    ((1, 6), (2, 5), (9, 4)),
    ((4, 9), (12, 8), (13, 7)),
    ((8, 12), (14, 11), (15, 10)),
    ((7, 13), (11, 14), (10, 15)),
)
HOP = 3
LAG = 4 * HOP + 1
STARTS = (LAG, CUTS + LAG, max(4 * CUTS, 2 * CUTS + LAG), 3 * CUTS + LAG, 4 * CUTS + LAG)
FIRST_ROWS = (0, 512, 896, 1280, 1664)
TURNS = STARTS[-1] + CUTS
DOTS = (
    STARTS[0] + 3, STARTS[0] + 7, STARTS[1] + 5, STARTS[2] + 2, STARTS[2] + 7,
    max(STARTS[3] + 5, STARTS[2] + 11), max(STARTS[4] + 2, STARTS[3] + 9), STARTS[4] + 7,
)


def base_of(block):
    return 128 + CUTS * TRIO * ((block - 1) // 3) + PIECE * ((block - 1) % 3)


def row_of(block, cut):
    return PIECE * cut if block == 0 else base_of(block) + TRIO * cut


def pick(choice, values):
    out = values[-1]
    for i in reversed(range(len(values) - 1)):
        out = jnp.where(choice == i, values[i], out)
    return out


def kernel(
    map_ref, weights_ref, mask_ref, total,
    store, relay, weights, mask, scales, columns, right_hi, right_lo, left_hi, left_lo,
    small_sem, load_sem, slot_sem, left_sem, relay_sem, scale_sem,
    sent_sem, sent_scale_sem, plus_sem, minus_sem, twin_sem, cross_sem, toward_sem, onward_sem,
):
    row, col = lax.axis_index("row"), lax.axis_index("col")
    x_lo, z = row // 8, row % 8
    x_hi, y, core = col // 8, (col // 2) % 4, col % 2
    up = (x_lo * 8 + (z + 1) % 8, col)
    down = (x_lo * 8 + (z + 7) % 8, col)
    pair = ((1 - x_lo) * 8 + z, col)
    twin = (row, x_hi * 8 + y * 2 + (1 - core))
    plus_0, plus = ((row, x_hi * 8 + ((y + 1) % 4) * 2 + n) for n in range(2))
    minus_0, minus = ((row, x_hi * 8 + ((y + 3) % 4) * 2 + n) for n in range(2))
    across_0, across = (((1 - x_lo) * 8 + z, (1 - x_hi) * 8 + y * 2 + n) for n in range(2))
    links = (up, down, pair)
    outer = x_hi == x_lo
    inner = x_hi != x_lo
    dy = (y + 4 - z // 2) % 4
    owner = (dy == 0) & (core == z % 2)
    first = jnp.where(outer & (dy == 0), core == z % 2, core == 1)

    def loading(cut):
        rows = pl.ds(PIECE * cut, PIECE)
        return pltpu.make_async_copy(map_ref.at[rows], store.at[rows], load_sem.at[cut])

    for cut in range(CUTS):
        loading(cut).start()
    small = (
        pltpu.make_async_copy(weights_ref, weights, small_sem.at[0]),
        pltpu.make_async_copy(mask_ref, mask, small_sem.at[1]),
    )
    for one in small:
        one.start()

    barrier = pltpu.get_barrier_semaphore()
    for other in (up, down, pair, twin, plus_0, plus, minus_0, minus, across_0, across):
        pl.semaphore_signal(barrier, inc=1, device_id=other, device_id_type=MESH)
    for one in small:
        one.wait()
    scales[pl.ds(0, 8), :] = jnp.broadcast_to(weights[...] * mask[...].astype(jnp.float32), (8, 128))
    pl.semaphore_wait(barrier, 10)

    def remote(source, target, sent, arrived, device):
        return pltpu.make_async_remote_copy(
            src_ref=source, dst_ref=target, send_sem=sent, recv_sem=arrived,
            device_id=device, device_id_type=MESH,
        )

    def arrival(ref, sem):
        return remote(ref, ref, sent_sem.at[0], sem, up)

    def span(start, size):
        return store.at[pl.ds(pl.multiple_of(start, 8), size)]

    def send_scale(source_block, step, g):
        remote(
            scales.at[pl.ds(8 * source_block, 8)],
            scales.at[pl.ds(pl.multiple_of(8 * (3 * step + 1 + g), 8), 8)],
            sent_scale_sem.at[0], scale_sem.at[step], links[g],
        ).start()

    for cut in range(CUTS):
        loading(cut).wait()
        if cut == 1:
            for g in range(3):
                send_scale(0, 0, g)
        for g in range(3):
            remote(
                span(PIECE * cut, PIECE), span(128 + TRIO * cut + PIECE * g, PIECE),
                sent_sem.at[0], slot_sem.at[cut], links[g],
            ).start()

    total[...] = jnp.zeros_like(total)

    def expand(block, start):
        square = jnp.broadcast_to(scales[pl.ds(pl.multiple_of(start, 8), 1), :], (128, 128))
        columns[block] = square.T

    back = (4 - dy) % 4
    hops = []
    for lane in range(4):
        on_outer = dy if lane % 2 == 0 else back
        on_inner = (1 + dy, 1 + back, pick(dy, (3, 2, 3, 4)), pick(dy, (3, 4, 3, 2)))[lane]
        hops.append(jnp.where(outer, on_outer, on_inner))
    goes_plus = (
        jnp.where(outer, dy <= 2, dy <= 2),
        inner & (dy < 0),
        jnp.where(outer, dy <= 2, (dy == 1) | (dy == 2)),
        inner & (dy == 3),
    )
    goes_minus = (
        inner & (dy < 0),
        jnp.where(outer, dy != 1, dy != 1),
        inner & (dy == 1),
        jnp.where(outer, dy != 1, (dy == 2) | (dy == 3)),
    )
    at_source = outer & owner
    from_row = jnp.where(at_source, 0, LEFT)

    def piece_of(slot, lane):
        third = (slot + 40 + lane) % 4
        there = (slot >= 0) & (slot < SLOTS) & ((third < 3) | (slot < CUTS))
        return jnp.where(third == 3, PIECE * slot, 128 + TRIO * slot + PIECE * third), there

    def pass_on(slot, lane, source_row, device, sent):
        at, _ = piece_of(slot, lane)
        remote(span(source_row + at, PIECE), span(LEFT + at, PIECE), sent, left_sem.at[lane, slot], device).start()

    def held(slot):
        return relay.at[pl.ds(pl.multiple_of(PIECE * slot, 8), PIECE)]

    def into_relay(slot, lane, device, sent):
        at, _ = piece_of(slot, lane)
        remote(span(at, PIECE), held(slot), sent, relay_sem.at[slot], device).start()

    def out_of_relay(slot, lane):
        at, _ = piece_of(slot, lane)
        arrival(held(slot), relay_sem.at[slot]).wait_recv()
        remote(held(slot), span(LEFT + at, PIECE), onward_sem.at[0], left_sem.at[lane, slot], across).start()

    def split(turn, start, phase, base, pieces):
        cut = turn - start

        @pl.when((turn >= start) & (turn < start + CUTS))
        def _():
            for n in range(pieces):
                (right_o, left_o), (right_i, left_i) = OUTER[phase][n], INNER[phase][n]

                def start_of(a, b):
                    def one(block):
                        return PIECE * cut if block == 0 else base_of(block) + TRIO * cut

                    return one(a) if a == b else jnp.where(outer, one(a), one(b))

                right_row = pl.multiple_of(start_of(right_o, right_i), 8)
                left_row = pl.multiple_of(LEFT + start_of(left_o, left_i), 8)
                block = right_o if right_o == right_i else jnp.where(outer, right_o, right_i)
                put = pl.ds(pl.multiple_of(base + PIECE * (pieces * cut + n), 16), PIECE)
                factor = columns[block, pl.ds(pl.multiple_of(PIECE * cut, 8), PIECE), :]
                for lane in range(SIDE // 128):
                    at = pl.ds(128 * lane, 128)
                    value = store[pl.ds(right_row, PIECE), at] * factor
                    high = value.astype(jnp.bfloat16)
                    right_hi[put, at] = high
                    right_lo[put, at] = (value - high.astype(jnp.float32)).astype(jnp.bfloat16)
                left_from = jnp.where(at_source, left_row - LEFT, left_row)
                value = store[pl.ds(pl.multiple_of(left_from, 8), PIECE), :]
                high = value.astype(jnp.bfloat16)
                left_hi[put, :] = high
                left_lo[put, :] = (value - high.astype(jnp.float32)).astype(jnp.bfloat16)

    def multiply(unit, n):
        k = pl.ds(pl.multiple_of(256 * unit, 256), 256)
        at = pl.ds(pl.multiple_of(256 * n, 256), 256)

        def product(a, b):
            return lax.dot_general(
                a[k, :], b[k, at], (((0,), (0,)), ((), ())), preferred_element_type=jnp.float32
            )

        total[:, at] += product(left_hi, right_hi) + product(left_hi, right_lo) + product(left_lo, right_hi)

    @pl.loop(0, TURNS)
    def _(turn):
        step, cut = turn // CUTS, turn % CUTS

        @pl.when(turn < SLOTS)
        def _():
            arrival(span(128 + TRIO * turn, TRIO), slot_sem.at[turn]).wait_recv()

            @pl.when(cut == 0)
            def _():
                arrival(scales.at[pl.ds(pl.multiple_of(8 + 24 * step, 8), 24)], scale_sem.at[step]).wait_recv()
                for g in range(3):
                    @pl.when(step < STEPS - 1)
                    def _():
                        source = pick(step, tuple(PARENT[s][g] for s in range(1, STEPS)))
                        remote(
                            scales.at[pl.ds(pl.multiple_of(8 * source, 8), 8)],
                            scales.at[pl.ds(pl.multiple_of(8 * (3 * step + 4 + g), 8), 8)],
                            sent_scale_sem.at[0], scale_sem.at[step + 1], links[g],
                        ).start()

            @pl.when(step < STEPS - 1)
            def _():
                for g in range(3):
                    base = pick(step, tuple(base_of(PARENT[s][g]) for s in range(1, STEPS)))
                    remote(
                        span(base + TRIO * cut, PIECE), span(128 + TRIO * (turn + CUTS) + PIECE * g, PIECE),
                        sent_sem.at[step + 1], slot_sem.at[turn + CUTS], links[g],
                    ).start()

            @pl.when(inner & owner)
            def _():
                for lane in range(4):
                    @pl.when(piece_of(turn, lane)[1])
                    def _():
                        if lane < 2:
                            pass_on(turn, lane, 0, across, cross_sem.at[0])
                        else:
                            into_relay(turn, lane, (plus, minus)[lane - 2], toward_sem.at[lane - 2])

        for lane, place in ((2, 1), (3, 3)):
            slot = turn - HOP

            @pl.when(inner & first & (dy == place) & piece_of(slot, lane)[1])
            def _():
                out_of_relay(slot, lane)

        for lane in range(4):
            slot = turn - HOP * hops[lane] - jnp.where(first, 0, 1)
            at, there = piece_of(slot, lane)

            @pl.when(there)
            def _():
                @pl.when(jnp.logical_not(at_source))
                def _():
                    arrival(span(LEFT + at, PIECE), left_sem.at[lane, slot]).wait_recv()

                @pl.when(first & goes_plus[lane])
                def _():
                    pass_on(slot, lane, from_row, plus, plus_sem.at[lane])

                @pl.when(first & goes_minus[lane])
                def _():
                    pass_on(slot, lane, from_row, minus, minus_sem.at[lane])

                @pl.when(first)
                def _():
                    pass_on(slot, lane, from_row, twin, twin_sem.at[lane])

        for phase, blocks in ((0, range(7)), (1, range(7, 10)), (2, range(10, 16))):
            @pl.when(turn == STARTS[phase])
            def _():
                for block in blocks:
                    expand(block, 8 * block)

        for phase in range(5):
            split(turn, STARTS[phase], phase, FIRST_ROWS[phase], len(OUTER[phase]))

        unit, begun = 0, DOTS[0]
        for number, at in enumerate(DOTS):
            unit = jnp.where(turn >= at, number, unit)
            begun = jnp.where(turn >= at, at, begun)
        quarter = turn - begun
        last = unit == len(DOTS) - 1

        @pl.when((quarter >= 0) & (quarter < 4))
        def _():
            @pl.loop(quarter, jnp.where(last, 4, quarter + 1))
            def _(n):
                multiply(unit, n)

    for step in range(STEPS):
        remote(
            span(0, CUTS * TRIO), span(0, CUTS * TRIO), sent_sem.at[step], slot_sem.at[0], up
        ).wait_send()
    remote(
        scales.at[pl.ds(8, 120)], scales.at[pl.ds(8, 120)], sent_scale_sem.at[0], slot_sem.at[0], up
    ).wait_send()

    def drain(sem, rows):
        remote(span(0, rows), span(0, rows), sem, slot_sem.at[0], up).wait_send()

    for lane in range(4):
        @pl.when(first & goes_plus[lane])
        def _():
            drain(plus_sem.at[lane], 512)

        @pl.when(first & goes_minus[lane])
        def _():
            drain(minus_sem.at[lane], 512)

        @pl.when(first)
        def _():
            drain(twin_sem.at[lane], 512)

    @pl.when(inner & owner)
    def _():
        drain(cross_sem.at[0], 1024)
        drain(toward_sem.at[0], 512)
        drain(toward_sem.at[1], 512)

    @pl.when(inner & first & ((dy == 1) | (dy == 3)))
    def _():
        drain(onward_sem.at[0], 512)


def per_device(forward_map, sensor_weights, sensor_mask):
    dma = pltpu.SemaphoreType.DMA
    half = pltpu.VMEM((OBS, SIDE), jnp.bfloat16)
    return pl.pallas_call(
        kernel,
        out_shape=pltpu.VMEM((SIDE, SIDE), jnp.float32),
        in_specs=[
            pl.BlockSpec(memory_space=pltpu.HBM),
            pl.BlockSpec(memory_space=pltpu.HBM),
            pl.BlockSpec(memory_space=pltpu.HBM),
        ],
        out_specs=pl.BlockSpec(memory_space=pltpu.VMEM),
        scratch_shapes=[
            pltpu.VMEM((2 * OBS, SIDE), jnp.float32),
            pltpu.VMEM((PIECE * SLOTS, SIDE), jnp.float32),
            pltpu.VMEM((1, 128), jnp.float32),
            pltpu.VMEM((1, 128), jnp.int32),
            pltpu.VMEM((128, 128), jnp.float32),
            pltpu.VMEM((16, 128, 128), jnp.float32),
            half, half, half, half,
            dma((2,)), dma((CUTS,)), dma((SLOTS,)), dma((4, SLOTS)), dma((SLOTS,)), dma((STEPS,)),
            dma((STEPS,)), dma((1,)), dma((4,)), dma((4,)), dma((4,)), dma((1,)), dma((2,)), dma((1,)),
        ],
        compiler_params=pltpu.CompilerParams(
            collective_id=0, has_side_effects=True, vmem_limit_bytes=67043328 - 4 * SIDE * SIDE
        ),
        cost_estimate=pl.CostEstimate(
            flops=2 * OBS * SIDE * SIDE, bytes_accessed=8 * SIDE * SIDE, transcendentals=0
        ),
    )(forward_map, sensor_weights.reshape(1, -1), sensor_mask.reshape(1, -1))


def solution(mesh):
    placed = (P("row", "col"), P("row"), P("row"))
    return jax.shard_map(
        per_device, mesh=mesh, in_specs=placed, out_specs=P("row", "col"), check_vma=False
    )
```

```python
import functools

import jax
import jax.numpy as jnp
from jax import lax
from jax.experimental import pallas as pl
from jax.experimental.pallas import tpu as pltpu
from jax.sharding import PartitionSpec as P

MESH = pl.DeviceIdType.MESH
OBS, SIDE = 2048, 1024
PIECE, STEPS, CUTS = 16, 5, 8
SLOTS = STEPS * CUTS
TRIO = 3 * PIECE
LEFT = OBS

PARENT = ((0, 0, 0), (1, 3, 1), (4, 2, 4), (7, 8, 8), (9, 12, 10))

OUTER = tuple(tuple((i, i) for i in blocks) for blocks in (range(4), range(4, 7), range(7, 9), range(9, 13), range(13, 16)))
INNER = (
    ((0, 3), (3, 0), (6, 1), (5, 2)),
    ((1, 6), (2, 5), (9, 4)),
    ((4, 9), (12, 8)),
    ((8, 12), (13, 7), (14, 11), (15, 10)),
    ((7, 13), (11, 14), (10, 15)),
)
WIDE = 256
LATE = 38
BEHIND = (0, 3, 5, 8, 10)
LAG = BEHIND[4] + 1
STARTS = (LAG, CUTS + LAG, 2 * CUTS + LAG, 3 * CUTS + LAG, 4 * CUTS + LAG)
FIRST_ROWS = (0, 512, 896, 1152, 1664)
SOONER = LAG - (BEHIND[3] + 1)
TURNS = STARTS[-1] + CUTS - SOONER


def rows_of(lane, first, end):
    return PIECE * sum(slot < CUTS or (slot + lane) % 4 < 3 for slot in range(first, end))


def dots():
    begun, out = 0, []
    for unit in range(7):
        rows = 256 * (unit + 1)
        group = max(n for n in range(5) if FIRST_ROWS[n] < rows)
        full = -(-(rows - FIRST_ROWS[group]) // (PIECE * len(OUTER[group])))
        begun = max(begun, STARTS[group] + full - 1)
        for quarter in range(4):
            out.append([begun + quarter, unit, quarter, 1])
        begun += 4
    out = [one for one in out if one[2] == 0 or one[0] >= TURNS - 1]
    out = [one for one in out if one[0] < TURNS - 1] + TAIL
    return tuple(map(tuple, out))


TAIL = [[TURNS - 2, 6, 2, 2]]
DOTS = dots()


def base_of(block):
    return 128 + CUTS * TRIO * ((block - 1) // 3) + PIECE * ((block - 1) % 3)


def row_of(block, cut):
    return PIECE * cut if block == 0 else base_of(block) + TRIO * cut


def pick(choice, values):
    out = values[-1]
    for i in reversed(range(len(values) - 1)):
        out = jnp.where(choice == i, values[i], out)
    return out


def products(unit, at, right_hi, right_lo, left_hi, left_lo):
    k = pl.ds(256 * unit if isinstance(unit, int) else pl.multiple_of(256 * unit, 256), 256)

    def product(a, b):
        return lax.dot_general(a[k, :], b[k, at], (((0,), (0,)), ((), ())), preferred_element_type=jnp.float32)

    return product(left_hi, right_hi) + product(left_hi, right_lo) + product(left_lo, right_hi)


def last_unit(total, right_hi, right_lo, left_hi, left_lo, gram_ref, done, out_sem):
    def writing(n):
        at = pl.ds(n * WIDE if isinstance(n, int) else pl.multiple_of(n * WIDE, WIDE), WIDE)
        return pltpu.make_async_copy(done.at[n], gram_ref.at[:, at], out_sem.at[n])

    @pl.loop(0, SIDE // WIDE)
    def _(n):
        at = pl.ds(pl.multiple_of(n * WIDE, WIDE), WIDE)
        done[n] = total[:, at] + products(7, at, right_hi, right_lo, left_hi, left_lo)
        writing(n).start()

    for n in range(SIDE // WIDE):
        writing(n).wait()


def kernel(
    map_ref, weights_ref, mask_ref, total, right_hi, right_lo, left_hi, left_lo,
    store, relay, weights, mask, scales, columns,
    small_sem, load_sem, slot_sem, left_sem, relay_sem, scale_sem,
    sent_sem, sent_scale_sem, plus_sem, minus_sem, twin_sem, cross_sem, toward_sem, onward_sem,
):
    row, col = lax.axis_index("row"), lax.axis_index("col")
    x_lo, z = row // 8, row % 8
    x_hi, y, core = col // 8, (col // 2) % 4, col % 2
    up = (x_lo * 8 + (z + 1) % 8, col)
    down = (x_lo * 8 + (z + 7) % 8, col)
    pair = ((1 - x_lo) * 8 + z, col)
    twin = (row, x_hi * 8 + y * 2 + (1 - core))
    plus_0, plus = ((row, x_hi * 8 + ((y + 1) % 4) * 2 + n) for n in range(2))
    minus_0, minus = ((row, x_hi * 8 + ((y + 3) % 4) * 2 + n) for n in range(2))
    across_0, across = (((1 - x_lo) * 8 + z, (1 - x_hi) * 8 + y * 2 + n) for n in range(2))
    links = (up, down, pair)
    outer = x_hi == x_lo
    inner = x_hi != x_lo
    dy = (y + 4 - z // 2) % 4
    owner = (dy == 0) & (core == z % 2)
    first = jnp.where(outer & (dy == 0), core == z % 2, core == 1)

    def loading(cut):
        rows = pl.ds(PIECE * cut, PIECE)
        return pltpu.make_async_copy(map_ref.at[rows], store.at[rows], load_sem.at[cut])

    for cut in range(CUTS):
        loading(cut).start()
    small = (
        pltpu.make_async_copy(weights_ref, weights, small_sem.at[0]),
        pltpu.make_async_copy(mask_ref, mask, small_sem.at[1]),
    )
    for one in small:
        one.start()

    barrier = pltpu.get_barrier_semaphore()
    for other in (up, down, pair, twin, plus_0, plus, minus_0, minus, across_0, across):
        pl.semaphore_signal(barrier, inc=1, device_id=other, device_id_type=MESH)
    for one in small:
        one.wait()
    scales[pl.ds(0, 8), :] = jnp.broadcast_to(weights[...] * mask[...].astype(jnp.float32), (8, 128))
    pl.semaphore_wait(barrier, 10)

    def remote(source, target, sent, arrived, device):
        return pltpu.make_async_remote_copy(
            src_ref=source, dst_ref=target, send_sem=sent, recv_sem=arrived,
            device_id=device, device_id_type=MESH,
        )

    def arrival(ref, sem):
        return remote(ref, ref, sent_sem.at[0], sem, up)

    def span(start, size):
        return store.at[pl.ds(pl.multiple_of(start, 8), size)]

    def send_scale(source_block, step, g):
        remote(
            scales.at[pl.ds(8 * source_block, 8)],
            scales.at[pl.ds(pl.multiple_of(8 * (3 * step + 1 + g), 8), 8)],
            sent_scale_sem.at[0], scale_sem.at[step], links[g],
        ).start()

    for cut in range(CUTS):
        loading(cut).wait()
        if cut == 1:
            for g in range(3):
                send_scale(0, 0, g)
        for g in range(3):
            remote(
                span(PIECE * cut, PIECE), span(128 + TRIO * cut + PIECE * g, PIECE),
                sent_sem.at[0], slot_sem.at[cut], links[g],
            ).start()

    total[...] = jnp.zeros_like(total)

    def expand(block, start):
        square = jnp.broadcast_to(scales[pl.ds(pl.multiple_of(start, 8), 1), :], (128, 128))
        columns[block] = square.T

    back = (4 - dy) % 4
    hops = []
    for lane in range(4):
        on_outer = dy if lane % 2 == 0 else back
        on_inner = (1 + dy, 1 + back, pick(dy, (3, 2, 3, 4)), pick(dy, (3, 4, 3, 2)))[lane]
        hops.append(jnp.where(outer, on_outer, on_inner))
    late = [pick(hop, BEHIND) + jnp.where(first, 0, 1) for hop in hops]
    goes_plus = (
        jnp.where(outer, dy <= 2, dy <= 2),
        inner & (dy < 0),
        jnp.where(outer, dy <= 2, (dy == 1) | (dy == 2)),
        inner & (dy == 3),
    )
    goes_minus = (
        inner & (dy < 0),
        jnp.where(outer, dy != 1, dy != 1),
        inner & (dy == 1),
        jnp.where(outer, dy != 1, (dy == 2) | (dy == 3)),
    )
    at_source = outer & owner
    late_hops = jnp.where(outer, pick(dy, (0, 1, 2, 1)), pick(dy, (1, 2, 3, 2)))
    late_by = pick(late_hops, BEHIND) + jnp.where(first, 0, 1)
    ends = first & (dy == 0)
    late_plus = (first & (dy <= 1), ends)
    late_minus = (ends, first & ((dy == 0) | (dy == 3)))
    from_row = jnp.where(at_source, 0, LEFT)
    waits = jnp.logical_not(at_source)
    relays = inner & first & ((dy == 1) | (dy == 3))
    crosses = inner & owner
    sends_plus = [first & one for one in goes_plus]
    sends_minus = [first & one for one in goes_minus]

    def piece_of(slot, lane):
        third = (slot + 40 + lane) & 3
        there = (slot >= 0) & (slot < SLOTS) & ((third < 3) | (slot < CUTS))
        return jnp.where(third == 3, PIECE * slot, 128 + TRIO * slot + PIECE * third), there

    def pass_on(slot, lane, at, source_row, device, sent):
        remote(span(source_row + at, PIECE), span(LEFT + at, PIECE), sent, left_sem.at[lane, slot], device).start()

    def held(slot):
        return relay.at[pl.ds(pl.multiple_of(PIECE * slot, 8), PIECE)]

    def into_relay(slot, at, device, sent):
        remote(span(at, PIECE), held(slot), sent, relay_sem.at[slot], device).start()

    def out_of_relay(slot, lane, at):
        arrival(held(slot), relay_sem.at[slot]).wait_recv()
        remote(held(slot), span(LEFT + at, PIECE), onward_sem.at[0], left_sem.at[lane, slot], across).start()

    def split(turn, start, phase, base, pieces, first_cut=0, end_cut=CUTS):
        cut = turn - start

        @pl.when((turn >= start + first_cut) & (turn < start + end_cut))
        def _():
            for n in range(pieces):
                (right_o, left_o), (right_i, left_i) = OUTER[phase][n], INNER[phase][n]

                def start_of(a, b):
                    def one(block):
                        return PIECE * cut if block == 0 else base_of(block) + TRIO * cut

                    return one(a) if a == b else jnp.where(outer, one(a), one(b))

                right_row = pl.multiple_of(start_of(right_o, right_i), 8)
                left_row = pl.multiple_of(LEFT + start_of(left_o, left_i), 8)
                block = right_o if right_o == right_i else jnp.where(outer, right_o, right_i)
                put = pl.ds(pl.multiple_of(base + PIECE * (pieces * cut + n), 16), PIECE)
                factor = columns[block, pl.ds(pl.multiple_of(PIECE * cut, 8), PIECE), :]
                for lane in range(SIDE // 128):
                    at = pl.ds(128 * lane, 128)
                    value = store[pl.ds(right_row, PIECE), at] * factor
                    high = value.astype(jnp.bfloat16)
                    right_hi[put, at] = high
                    right_lo[put, at] = (value - high.astype(jnp.float32)).astype(jnp.bfloat16)
                left_from = jnp.where(at_source, left_row - LEFT, left_row)
                value = store[pl.ds(pl.multiple_of(left_from, 8), PIECE), :]
                high = value.astype(jnp.bfloat16)
                left_hi[put, :] = high
                left_lo[put, :] = (value - high.astype(jnp.float32)).astype(jnp.bfloat16)

    def multiply(unit, n):
        at = pl.ds(pl.multiple_of(256 * n, 256), 256)
        total[:, at] += products(unit, at, right_hi, right_lo, left_hi, left_lo)

    @pl.loop(0, TURNS)
    def _(turn):
        step, cut = turn >> 3, turn & 7

        @pl.when(turn < SLOTS)
        def _():
            arrival(span(128 + TRIO * turn, TRIO), slot_sem.at[turn]).wait_recv()

            @pl.when(cut == 0)
            def _():
                arrival(scales.at[pl.ds(pl.multiple_of(8 + 24 * step, 8), 24)], scale_sem.at[step]).wait_recv()
                for g in range(3):
                    @pl.when(step < STEPS - 1)
                    def _():
                        source = pick(step, tuple(PARENT[s][g] for s in range(1, STEPS)))
                        remote(
                            scales.at[pl.ds(pl.multiple_of(8 * source, 8), 8)],
                            scales.at[pl.ds(pl.multiple_of(8 * (3 * step + 4 + g), 8), 8)],
                            sent_scale_sem.at[0], scale_sem.at[step + 1], links[g],
                        ).start()

            @pl.when(step < STEPS - 1)
            def _():
                for g in range(3):
                    base = pick(step, tuple(base_of(PARENT[s][g]) for s in range(1, STEPS)))
                    remote(
                        span(base + TRIO * cut, PIECE), span(128 + TRIO * (turn + CUTS) + PIECE * g, PIECE),
                        sent_sem.at[step + 1], slot_sem.at[turn + CUTS], links[g],
                    ).start()

            @pl.when(crosses)
            def _():
                for lane in range(4):
                    at, there = piece_of(turn, lane)

                    @pl.when(there)
                    def _():
                        @pl.when(turn >= LATE)
                        def _():
                            pass_on(turn, lane, at, 0, across, cross_sem.at[1])

                        @pl.when(turn < LATE)
                        def _():
                            if lane < 2:
                                pass_on(turn, lane, at, 0, across, cross_sem.at[0])
                            else:
                                into_relay(turn, at, (plus, minus)[lane - 2], toward_sem.at[lane - 2])

        @pl.when(relays)
        def _():
            slot = turn - BEHIND[1]
            for lane, place in ((2, 1), (3, 3)):
                at, there = piece_of(slot, lane)

                @pl.when((dy == place) & there & (slot < LATE))
                def _():
                    out_of_relay(slot, lane, at)

        def forward(slot, lane, at, on_plus, on_minus, sems):
            @pl.when(waits)
            def _():
                arrival(span(LEFT + at, PIECE), left_sem.at[lane, slot]).wait_recv()

            @pl.when(on_plus)
            def _():
                pass_on(slot, lane, at, from_row, plus, plus_sem.at[sems + lane])

            @pl.when(on_minus)
            def _():
                pass_on(slot, lane, at, from_row, minus, minus_sem.at[sems + lane])

            @pl.when(first)
            def _():
                pass_on(slot, lane, at, from_row, twin, twin_sem.at[lane])

        @pl.when((turn - late_by >= LATE) & (turn - late_by < SLOTS))
        def _():
            slot = turn - late_by
            for lane in range(4):
                at, there = piece_of(slot, lane)

                @pl.when(there)
                def _():
                    forward(slot, lane, at, late_plus[lane % 2], late_minus[lane % 2], 4)

        for lane in range(4):
            slot = turn - late[lane]
            at, there = piece_of(slot, lane)

            @pl.when(there & (slot < LATE))
            def _():
                forward(slot, lane, at, sends_plus[lane], sends_minus[lane], 0)

        for phase, blocks in ((0, range(7)), (1, range(7, 10)), (2, range(10, 13)), (3, range(13, 16))):
            @pl.when(turn == STARTS[phase])
            def _():
                for block in blocks:
                    expand(block, 8 * block)

        late_cut = LATE % CUTS
        for phase in range(4):
            split(turn, STARTS[phase], phase, FIRST_ROWS[phase], len(OUTER[phase]))
        split(turn, STARTS[4], 4, FIRST_ROWS[4], len(OUTER[4]), 0, late_cut)
        split(turn, STARTS[4] - SOONER, 4, FIRST_ROWS[4], len(OUTER[4]), late_cut, CUTS)

        begun, unit, ahead, pace = DOTS[0]
        for one in DOTS[1:]:
            begun, unit, ahead, pace = (jnp.where(turn >= one[0], new, old) for new, old in zip(one, (begun, unit, ahead, pace)))
        quarter = ahead + pace * (turn - begun)

        @pl.when((quarter >= 0) & (quarter < 4))
        def _():
            @pl.loop(quarter, quarter + pace)
            def _(n):
                multiply(unit, n)

    for step in range(STEPS):
        remote(
            span(0, CUTS * TRIO), span(0, CUTS * TRIO), sent_sem.at[step], slot_sem.at[0], up
        ).wait_send()
    remote(
        scales.at[pl.ds(8, 120)], scales.at[pl.ds(8, 120)], sent_scale_sem.at[0], slot_sem.at[0], up
    ).wait_send()

    def drain(sem, rows):
        remote(span(0, rows), span(0, rows), sem, slot_sem.at[0], up).wait_send()

    for lane in range(4):
        soon, later = rows_of(lane, 0, LATE), rows_of(lane, LATE, SLOTS)
        for condition, sem, rows in (
            (sends_plus[lane], plus_sem.at[lane], soon),
            (sends_minus[lane], minus_sem.at[lane], soon),
            (late_plus[lane % 2], plus_sem.at[4 + lane], later),
            (late_minus[lane % 2], minus_sem.at[4 + lane], later),
            (first, twin_sem.at[lane], soon + later),
        ):
            @pl.when(condition)
            def _():
                drain(sem, rows)

    @pl.when(crosses)
    def _():
        drain(cross_sem.at[0], rows_of(0, 0, LATE) + rows_of(1, 0, LATE))
        drain(cross_sem.at[1], sum(rows_of(lane, LATE, SLOTS) for lane in range(4)))
        drain(toward_sem.at[0], rows_of(2, 0, LATE))
        drain(toward_sem.at[1], rows_of(3, 0, LATE))

    for lane, place in ((2, 1), (3, 3)):
        @pl.when(relays & (dy == place))
        def _():
            drain(onward_sem.at[0], rows_of(lane, 0, LATE))


def per_device(forward_map, sensor_weights, sensor_mask):
    dma = pltpu.SemaphoreType.DMA
    half = pltpu.VMEM((OBS, SIDE), jnp.bfloat16)
    parts = pl.pallas_call(
        kernel,
        out_shape=(pltpu.VMEM((SIDE, SIDE), jnp.float32), half, half, half, half),
        in_specs=[
            pl.BlockSpec(memory_space=pltpu.HBM),
            pl.BlockSpec(memory_space=pltpu.HBM),
            pl.BlockSpec(memory_space=pltpu.HBM),
        ],
        out_specs=(pl.BlockSpec(memory_space=pltpu.VMEM),) * 5,
        scratch_shapes=[
            pltpu.VMEM((2 * OBS, SIDE), jnp.float32),
            pltpu.VMEM((PIECE * SLOTS, SIDE), jnp.float32),
            pltpu.VMEM((1, 128), jnp.float32),
            pltpu.VMEM((1, 128), jnp.int32),
            pltpu.VMEM((128, 128), jnp.float32),
            pltpu.VMEM((16, 128, 128), jnp.float32),
            dma((2,)), dma((CUTS,)), dma((SLOTS,)), dma((4, SLOTS)), dma((SLOTS,)), dma((STEPS,)),
            dma((STEPS,)), dma((1,)), dma((8,)), dma((8,)), dma((4,)), dma((2,)), dma((2,)), dma((1,)),
        ],
        compiler_params=pltpu.CompilerParams(
            collective_id=0, has_side_effects=True, vmem_limit_bytes=67043328 - 20 * SIDE * SIDE
        ),
        cost_estimate=pl.CostEstimate(
            flops=2 * OBS * SIDE * SIDE, bytes_accessed=8 * SIDE * SIDE, transcendentals=0
        ),
    )(forward_map, sensor_weights.reshape(1, -1), sensor_mask.reshape(1, -1))
    return pl.pallas_call(
        last_unit,
        out_shape=jax.ShapeDtypeStruct((SIDE, SIDE), jnp.float32),
        in_specs=[pl.BlockSpec(memory_space=pltpu.VMEM)] * 5,
        out_specs=pl.BlockSpec(memory_space=pl.ANY),
        scratch_shapes=[pltpu.VMEM((SIDE // WIDE, SIDE, WIDE), jnp.float32), dma((SIDE // WIDE,))],
        compiler_params=pltpu.CompilerParams(vmem_limit_bytes=16 * 1024 * 1024),
        cost_estimate=pl.CostEstimate(flops=2 * 256 * SIDE * SIDE, bytes_accessed=4 * SIDE * SIDE, transcendentals=0),
    )(*parts)


def solution(mesh):
    placed = (P("row", "col"), P("row"), P("row"))
    return jax.shard_map(
        per_device, mesh=mesh, in_specs=placed, out_specs=P("row", "col"), check_vma=False
    )
```

```python
import functools

import jax
import jax.numpy as jnp
from jax import lax
from jax.experimental import pallas as pl
from jax.experimental.pallas import tpu as pltpu
from jax.sharding import PartitionSpec as P

MESH = pl.DeviceIdType.MESH
OBS, SIDE = 2048, 1024
PIECE, STEPS, CUTS = 16, 5, 8
SLOTS = STEPS * CUTS
TRIO = 3 * PIECE
LEFT = OBS

PARENT = ((0, 0, 0), (1, 3, 1), (4, 2, 4), (7, 8, 8), (9, 12, 10))

OUTER = tuple(tuple((i, i) for i in blocks) for blocks in (range(4), range(4, 7), range(7, 9), range(9, 13), range(13, 16)))
INNER = (
    ((0, 3), (3, 0), (6, 1), (5, 2)),
    ((1, 6), (2, 5), (9, 4)),
    ((4, 9), (12, 8)),
    ((8, 12), (13, 7), (14, 11), (15, 10)),
    ((7, 13), (11, 14), (10, 15)),
)
WIDE = 512
LATE = 38
BEHIND = (0, 3, 5, 8, 10)
LAG = BEHIND[4] + 1
STARTS = (LAG, CUTS + LAG, 2 * CUTS + LAG, 3 * CUTS + LAG, 4 * CUTS + LAG)
FIRST_ROWS = (0, 512, 896, 1152, 1664)
SOONER = LAG - (BEHIND[3] + 1)
TURNS = STARTS[-1] + CUTS - SOONER


def rows_of(lane, first, end):
    return PIECE * sum(slot < CUTS or (slot + lane) % 4 < 3 for slot in range(first, end))


def dots():
    begun, out = 0, []
    for unit in range(7):
        rows = 256 * (unit + 1)
        group = max(n for n in range(5) if FIRST_ROWS[n] < rows)
        full = -(-(rows - FIRST_ROWS[group]) // (PIECE * len(OUTER[group])))
        begun = max(begun, STARTS[group] + full - 1)
        for quarter in range(4):
            out.append([begun + quarter, unit, quarter, 1])
        begun += 4
    out = [one for one in out if one[2] == 0 or one[0] >= TURNS - 1]
    out = [one for one in out if one[0] < TURNS - 1] + TAIL
    return tuple(map(tuple, out))


TAIL = [[TURNS - 2, 6, 2, 2]]
DOTS = dots()


def base_of(block):
    return 128 + CUTS * TRIO * ((block - 1) // 3) + PIECE * ((block - 1) % 3)


def row_of(block, cut):
    return PIECE * cut if block == 0 else base_of(block) + TRIO * cut


def pick(choice, values):
    out = values[-1]
    for i in reversed(range(len(values) - 1)):
        out = jnp.where(choice == i, values[i], out)
    return out


def products(unit, at, right_hi, right_lo, left_hi, left_lo):
    k = pl.ds(256 * unit if isinstance(unit, int) else pl.multiple_of(256 * unit, 256), 256)

    def product(a, b):
        return lax.dot_general(a[k, :], b[k, at], (((0,), (0,)), ((), ())), preferred_element_type=jnp.float32)

    return product(left_hi, right_hi) + product(left_hi, right_lo) + product(left_lo, right_hi)


def last_unit(total, right_hi, right_lo, left_hi, left_lo, gram_ref, done, out_sem):
    def writing(n):
        at = pl.ds(n * WIDE if isinstance(n, int) else pl.multiple_of(n * WIDE, WIDE), WIDE)
        return pltpu.make_async_copy(done.at[n], gram_ref.at[:, at], out_sem.at[n])

    @pl.loop(0, SIDE // WIDE)
    def _(n):
        at = pl.ds(pl.multiple_of(n * WIDE, WIDE), WIDE)
        done[n] = total[:, at] + products(7, at, right_hi, right_lo, left_hi, left_lo)
        writing(n).start()

    for n in range(SIDE // WIDE):
        writing(n).wait()


def kernel(
    map_ref, weights_ref, mask_ref, total, right_hi, right_lo, left_hi, left_lo,
    store, relay, weights, mask, scales, columns,
    small_sem, load_sem, slot_sem, left_sem, relay_sem, scale_sem,
    sent_sem, sent_scale_sem, plus_sem, minus_sem, twin_sem, cross_sem, toward_sem, onward_sem,
):
    row, col = lax.axis_index("row"), lax.axis_index("col")
    x_lo, z = row // 8, row % 8
    x_hi, y, core = col // 8, (col // 2) % 4, col % 2
    up = (x_lo * 8 + (z + 1) % 8, col)
    down = (x_lo * 8 + (z + 7) % 8, col)
    pair = ((1 - x_lo) * 8 + z, col)
    twin = (row, x_hi * 8 + y * 2 + (1 - core))
    plus_0, plus = ((row, x_hi * 8 + ((y + 1) % 4) * 2 + n) for n in range(2))
    minus_0, minus = ((row, x_hi * 8 + ((y + 3) % 4) * 2 + n) for n in range(2))
    across_0, across = (((1 - x_lo) * 8 + z, (1 - x_hi) * 8 + y * 2 + n) for n in range(2))
    links = (up, down, pair)
    outer = x_hi == x_lo
    inner = x_hi != x_lo
    dy = (y + 4 - z // 2) % 4
    owner = (dy == 0) & (core == z % 2)
    first = jnp.where(outer & (dy == 0), core == z % 2, core == 1)

    def loading(cut):
        rows = pl.ds(PIECE * cut, PIECE)
        return pltpu.make_async_copy(map_ref.at[rows], store.at[rows], load_sem.at[cut])

    for cut in range(CUTS):
        loading(cut).start()
    small = (
        pltpu.make_async_copy(weights_ref, weights, small_sem.at[0]),
        pltpu.make_async_copy(mask_ref, mask, small_sem.at[1]),
    )
    for one in small:
        one.start()

    barrier = pltpu.get_barrier_semaphore()
    for other in (up, down, pair, twin, plus_0, plus, minus_0, minus, across_0, across):
        pl.semaphore_signal(barrier, inc=1, device_id=other, device_id_type=MESH)
    for one in small:
        one.wait()
    scales[pl.ds(0, 8), :] = jnp.broadcast_to(weights[...] * mask[...].astype(jnp.float32), (8, 128))
    pl.semaphore_wait(barrier, 10)

    def remote(source, target, sent, arrived, device):
        return pltpu.make_async_remote_copy(
            src_ref=source, dst_ref=target, send_sem=sent, recv_sem=arrived,
            device_id=device, device_id_type=MESH,
        )

    def arrival(ref, sem):
        return remote(ref, ref, sent_sem.at[0], sem, up)

    def span(start, size):
        return store.at[pl.ds(pl.multiple_of(start, 8), size)]

    def send_scale(source_block, step, g):
        remote(
            scales.at[pl.ds(8 * source_block, 8)],
            scales.at[pl.ds(pl.multiple_of(8 * (3 * step + 1 + g), 8), 8)],
            sent_scale_sem.at[0], scale_sem.at[step], links[g],
        ).start()

    for cut in range(CUTS):
        loading(cut).wait()
        if cut == 1:
            for g in range(3):
                send_scale(0, 0, g)
        for g in range(3):
            remote(
                span(PIECE * cut, PIECE), span(128 + TRIO * cut + PIECE * g, PIECE),
                sent_sem.at[0], slot_sem.at[cut], links[g],
            ).start()

    total[...] = jnp.zeros_like(total)

    def expand(block, start):
        square = jnp.broadcast_to(scales[pl.ds(pl.multiple_of(start, 8), 1), :], (128, 128))
        columns[block] = square.T

    back = (4 - dy) % 4
    hops = []
    for lane in range(4):
        on_outer = dy if lane % 2 == 0 else back
        on_inner = (1 + dy, 1 + back, pick(dy, (3, 2, 3, 4)), pick(dy, (3, 4, 3, 2)))[lane]
        hops.append(jnp.where(outer, on_outer, on_inner))
    late = [pick(hop, BEHIND) + jnp.where(first, 0, 1) for hop in hops]
    goes_plus = (
        jnp.where(outer, dy <= 2, dy <= 2),
        inner & (dy < 0),
        jnp.where(outer, dy <= 2, (dy == 1) | (dy == 2)),
        inner & (dy == 3),
    )
    goes_minus = (
        inner & (dy < 0),
        jnp.where(outer, dy != 1, dy != 1),
        inner & (dy == 1),
        jnp.where(outer, dy != 1, (dy == 2) | (dy == 3)),
    )
    at_source = outer & owner
    late_hops = jnp.where(outer, pick(dy, (0, 1, 2, 1)), pick(dy, (1, 2, 3, 2)))
    late_by = pick(late_hops, BEHIND) + jnp.where(first, 0, 1)
    ends = first & (dy == 0)
    late_plus = (first & (dy <= 1), ends)
    late_minus = (ends, first & ((dy == 0) | (dy == 3)))
    from_row = jnp.where(at_source, 0, LEFT)
    waits = jnp.logical_not(at_source)
    relays = inner & first & ((dy == 1) | (dy == 3))
    crosses = inner & owner
    sends_plus = [first & one for one in goes_plus]
    sends_minus = [first & one for one in goes_minus]

    def piece_of(slot, lane):
        third = (slot + 40 + lane) & 3
        there = (slot >= 0) & (slot < SLOTS) & ((third < 3) | (slot < CUTS))
        return jnp.where(third == 3, PIECE * slot, 128 + TRIO * slot + PIECE * third), there

    def pass_on(slot, lane, at, source_row, device, sent):
        remote(span(source_row + at, PIECE), span(LEFT + at, PIECE), sent, left_sem.at[lane, slot], device).start()

    def held(slot):
        return relay.at[pl.ds(pl.multiple_of(PIECE * slot, 8), PIECE)]

    def into_relay(slot, at, device, sent):
        remote(span(at, PIECE), held(slot), sent, relay_sem.at[slot], device).start()

    def out_of_relay(slot, lane, at):
        arrival(held(slot), relay_sem.at[slot]).wait_recv()
        remote(held(slot), span(LEFT + at, PIECE), onward_sem.at[0], left_sem.at[lane, slot], across).start()

    def split(turn, start, phase, base, pieces, first_cut=0, end_cut=CUTS):
        cut = turn - start

        @pl.when((turn >= start + first_cut) & (turn < start + end_cut))
        def _():
            for n in range(pieces):
                (right_o, left_o), (right_i, left_i) = OUTER[phase][n], INNER[phase][n]

                def start_of(a, b):
                    def one(block):
                        return PIECE * cut if block == 0 else base_of(block) + TRIO * cut

                    return one(a) if a == b else jnp.where(outer, one(a), one(b))

                right_row = pl.multiple_of(start_of(right_o, right_i), 8)
                left_row = pl.multiple_of(LEFT + start_of(left_o, left_i), 8)
                block = right_o if right_o == right_i else jnp.where(outer, right_o, right_i)
                put = pl.ds(pl.multiple_of(base + PIECE * (pieces * cut + n), 16), PIECE)
                factor = columns[block, pl.ds(pl.multiple_of(PIECE * cut, 8), PIECE), :]
                for lane in range(SIDE // 128):
                    at = pl.ds(128 * lane, 128)
                    value = store[pl.ds(right_row, PIECE), at] * factor
                    high = value.astype(jnp.bfloat16)
                    right_hi[put, at] = high
                    right_lo[put, at] = (value - high.astype(jnp.float32)).astype(jnp.bfloat16)
                left_from = jnp.where(at_source, left_row - LEFT, left_row)
                value = store[pl.ds(pl.multiple_of(left_from, 8), PIECE), :]
                high = value.astype(jnp.bfloat16)
                left_hi[put, :] = high
                left_lo[put, :] = (value - high.astype(jnp.float32)).astype(jnp.bfloat16)

    def multiply(unit, n):
        at = pl.ds(pl.multiple_of(256 * n, 256), 256)
        total[:, at] += products(unit, at, right_hi, right_lo, left_hi, left_lo)

    def gathering(turn):
        step, cut = turn >> 3, turn & 7
        arrival(span(128 + TRIO * turn, TRIO), slot_sem.at[turn]).wait_recv()

        @pl.when(cut == 0)
        def _():
            arrival(scales.at[pl.ds(pl.multiple_of(8 + 24 * step, 8), 24)], scale_sem.at[step]).wait_recv()
            for g in range(3):
                @pl.when(step < STEPS - 1)
                def _():
                    source = pick(step, tuple(PARENT[s][g] for s in range(1, STEPS)))
                    remote(
                        scales.at[pl.ds(pl.multiple_of(8 * source, 8), 8)],
                        scales.at[pl.ds(pl.multiple_of(8 * (3 * step + 4 + g), 8), 8)],
                        sent_scale_sem.at[0], scale_sem.at[step + 1], links[g],
                    ).start()

        @pl.when(step < STEPS - 1)
        def _():
            for g in range(3):
                base = pick(step, tuple(base_of(PARENT[s][g]) for s in range(1, STEPS)))
                remote(
                    span(base + TRIO * cut, PIECE), span(128 + TRIO * (turn + CUTS) + PIECE * g, PIECE),
                    sent_sem.at[step + 1], slot_sem.at[turn + CUTS], links[g],
                ).start()

        @pl.when(crosses)
        def _():
            for lane in range(4):
                at, there = piece_of(turn, lane)

                @pl.when(there)
                def _():
                    @pl.when(turn >= LATE)
                    def _():
                        pass_on(turn, lane, at, 0, across, cross_sem.at[1])

                    @pl.when(turn < LATE)
                    def _():
                        if lane < 2:
                            pass_on(turn, lane, at, 0, across, cross_sem.at[0])
                        else:
                            into_relay(turn, at, (plus, minus)[lane - 2], toward_sem.at[lane - 2])

    def rest_of(turn, first_turn, end_turn):
        @pl.when(relays)
        def _():
            slot = turn - BEHIND[1]
            for lane, place in ((2, 1), (3, 3)):
                at, there = piece_of(slot, lane)

                @pl.when((dy == place) & there & (slot < LATE))
                def _():
                    out_of_relay(slot, lane, at)

        def forward(slot, lane, at, on_plus, on_minus, sems):
            @pl.when(waits)
            def _():
                arrival(span(LEFT + at, PIECE), left_sem.at[lane, slot]).wait_recv()

            @pl.when(on_plus)
            def _():
                pass_on(slot, lane, at, from_row, plus, plus_sem.at[sems + lane])

            @pl.when(on_minus)
            def _():
                pass_on(slot, lane, at, from_row, minus, minus_sem.at[sems + lane])

            @pl.when(first)
            def _():
                pass_on(slot, lane, at, from_row, twin, twin_sem.at[lane])

        is_late = (turn - late_by >= LATE) & (turn - late_by < SLOTS)

        @pl.when(is_late)
        def _():
            slot = turn - late_by
            for lane in range(4):
                at, there = piece_of(slot, lane)

                @pl.when(there)
                def _():
                    forward(slot, lane, at, late_plus[lane % 2], late_minus[lane % 2], 4)

        for lane in range(4):
            slot = turn - late[lane]
            at, there = piece_of(slot, lane)

            @pl.when(there & (slot < LATE))
            def _():
                forward(slot, lane, at, sends_plus[lane], sends_minus[lane], 0)

        for phase, blocks in ((0, range(7)), (1, range(7, 10)), (2, range(10, 13)), (3, range(13, 16))):
            if first_turn <= STARTS[phase] < end_turn:
                @pl.when(turn == STARTS[phase])
                def _():
                    for block in blocks:
                        expand(block, 8 * block)

        late_cut = LATE % CUTS
        for phase, sooner, first_cut, end_cut in (
            (0, 0, 0, CUTS), (1, 0, 0, CUTS), (2, 0, 0, CUTS), (3, 0, 0, CUTS),
            (4, 0, 0, late_cut), (4, SOONER, late_cut, CUTS),
        ):
            start = STARTS[phase] - sooner
            if start + first_cut < end_turn and start + end_cut > first_turn:
                split(turn, start, phase, FIRST_ROWS[phase], len(OUTER[phase]), first_cut, end_cut)

        dots_here = [one for n, one in enumerate(DOTS) if one[0] < end_turn and (n + 1 == len(DOTS) or DOTS[n + 1][0] > first_turn)]
        begun, unit, ahead, pace = dots_here[0]
        for one in dots_here[1:]:
            begun, unit, ahead, pace = (jnp.where(turn >= one[0], new, old) for new, old in zip(one, (begun, unit, ahead, pace)))
        quarter = ahead + pace * (turn - begun)

        @pl.when((quarter >= 0) & (quarter < 4))
        def _():
            @pl.loop(quarter, quarter + pace)
            def _(n):
                multiply(unit, n)

    @pl.loop(0, SLOTS)
    def _(turn):
        gathering(turn)
        rest_of(turn, 0, SLOTS)

    @pl.loop(SLOTS, TURNS)
    def _(turn):
        rest_of(turn, SLOTS, TURNS)

    for step in range(STEPS):
        remote(
            span(0, CUTS * TRIO), span(0, CUTS * TRIO), sent_sem.at[step], slot_sem.at[0], up
        ).wait_send()
    remote(
        scales.at[pl.ds(8, 120)], scales.at[pl.ds(8, 120)], sent_scale_sem.at[0], slot_sem.at[0], up
    ).wait_send()

    def drain(sem, rows):
        remote(span(0, rows), span(0, rows), sem, slot_sem.at[0], up).wait_send()

    for lane in range(4):
        soon, later = rows_of(lane, 0, LATE), rows_of(lane, LATE, SLOTS)
        for condition, sem, rows in (
            (sends_plus[lane], plus_sem.at[lane], soon),
            (sends_minus[lane], minus_sem.at[lane], soon),
            (late_plus[lane % 2], plus_sem.at[4 + lane], later),
            (late_minus[lane % 2], minus_sem.at[4 + lane], later),
            (first, twin_sem.at[lane], soon + later),
        ):
            @pl.when(condition)
            def _():
                drain(sem, rows)

    @pl.when(crosses)
    def _():
        drain(cross_sem.at[0], rows_of(0, 0, LATE) + rows_of(1, 0, LATE))
        drain(cross_sem.at[1], sum(rows_of(lane, LATE, SLOTS) for lane in range(4)))
        drain(toward_sem.at[0], rows_of(2, 0, LATE))
        drain(toward_sem.at[1], rows_of(3, 0, LATE))

    for lane, place in ((2, 1), (3, 3)):
        @pl.when(relays & (dy == place))
        def _():
            drain(onward_sem.at[0], rows_of(lane, 0, LATE))


def per_device(forward_map, sensor_weights, sensor_mask):
    dma = pltpu.SemaphoreType.DMA
    half = pltpu.VMEM((OBS, SIDE), jnp.bfloat16)
    parts = pl.pallas_call(
        kernel,
        out_shape=(pltpu.VMEM((SIDE, SIDE), jnp.float32), half, half, half, half),
        in_specs=[
            pl.BlockSpec(memory_space=pltpu.HBM),
            pl.BlockSpec(memory_space=pltpu.HBM),
            pl.BlockSpec(memory_space=pltpu.HBM),
        ],
        out_specs=(pl.BlockSpec(memory_space=pltpu.VMEM),) * 5,
        scratch_shapes=[
            pltpu.VMEM((2 * OBS, SIDE), jnp.float32),
            pltpu.VMEM((PIECE * SLOTS, SIDE), jnp.float32),
            pltpu.VMEM((1, 128), jnp.float32),
            pltpu.VMEM((1, 128), jnp.int32),
            pltpu.VMEM((128, 128), jnp.float32),
            pltpu.VMEM((16, 128, 128), jnp.float32),
            dma((2,)), dma((CUTS,)), dma((SLOTS,)), dma((4, SLOTS)), dma((SLOTS,)), dma((STEPS,)),
            dma((STEPS,)), dma((1,)), dma((8,)), dma((8,)), dma((4,)), dma((2,)), dma((2,)), dma((1,)),
        ],
        compiler_params=pltpu.CompilerParams(
            collective_id=0, has_side_effects=True, vmem_limit_bytes=67043328 - 20 * SIDE * SIDE
        ),
        cost_estimate=pl.CostEstimate(
            flops=2 * OBS * SIDE * SIDE, bytes_accessed=8 * SIDE * SIDE, transcendentals=0
        ),
    )(forward_map, sensor_weights.reshape(1, -1), sensor_mask.reshape(1, -1))
    return pl.pallas_call(
        last_unit,
        out_shape=jax.ShapeDtypeStruct((SIDE, SIDE), jnp.float32),
        in_specs=[pl.BlockSpec(memory_space=pltpu.VMEM)] * 5,
        out_specs=pl.BlockSpec(memory_space=pl.ANY),
        scratch_shapes=[pltpu.VMEM((SIDE // WIDE, SIDE, WIDE), jnp.float32), dma((SIDE // WIDE,))],
        compiler_params=pltpu.CompilerParams(vmem_limit_bytes=16 * 1024 * 1024),
        cost_estimate=pl.CostEstimate(flops=2 * 256 * SIDE * SIDE, bytes_accessed=4 * SIDE * SIDE, transcendentals=0),
    )(*parts)


def solution(mesh):
    placed = (P("row", "col"), P("row"), P("row"))
    return jax.shard_map(
        per_device, mesh=mesh, in_specs=placed, out_specs=P("row", "col"), check_vma=False
    )
```

```python
import functools

import jax
import jax.numpy as jnp
from jax import lax
from jax.experimental import pallas as pl
from jax.experimental.pallas import tpu as pltpu
from jax.sharding import PartitionSpec as P

MESH = pl.DeviceIdType.MESH
OBS, SIDE = 2048, 1024
PIECE, STEPS, CUTS = 16, 5, 8
SLOTS = STEPS * CUTS
TRIO = 3 * PIECE
LEFT = OBS

PARENT = ((0, 0, 0), (1, 3, 1), (4, 2, 4), (7, 8, 8), (9, 12, 10))

OUTER = tuple(tuple((i, i) for i in blocks) for blocks in (range(4), range(4, 7), range(7, 9), range(9, 13), range(13, 16)))
INNER = (
    ((0, 3), (3, 0), (6, 1), (5, 2)),
    ((1, 6), (2, 5), (9, 4)),
    ((4, 9), (12, 8)),
    ((8, 12), (13, 7), (14, 11), (15, 10)),
    ((7, 13), (11, 14), (10, 15)),
)
WIDE = 512
LATE = 38
BEHIND = (0, 3, 5, 8, 10)
LAG = BEHIND[4] + 1
STARTS = (LAG, CUTS + LAG, 2 * CUTS + LAG, 3 * CUTS + LAG, 4 * CUTS + LAG)
FIRST_ROWS = (0, 512, 896, 1152, 1664)
SOONER = LAG - (BEHIND[3] + 1)
TURNS = STARTS[-1] + CUTS - SOONER


def rows_of(lane, first, end):
    return PIECE * sum(slot < CUTS or (slot + lane) % 4 < 3 for slot in range(first, end))


def dots():
    begun, out = 0, []
    for unit in range(7):
        rows = 256 * (unit + 1)
        group = max(n for n in range(5) if FIRST_ROWS[n] < rows)
        full = -(-(rows - FIRST_ROWS[group]) // (PIECE * len(OUTER[group])))
        begun = max(begun, STARTS[group] + full - 1)
        for quarter in range(4):
            out.append([begun + quarter, unit, quarter, 1])
        begun += 4
    out = [one for one in out if one[2] == 0 or one[0] >= TURNS - 1]
    out = [one for one in out if one[0] < TURNS - 1] + TAIL
    return tuple(map(tuple, out))


TAIL = [[TURNS - 2, 6, 2, 2]]
DOTS = dots()


def base_of(block):
    return 128 + CUTS * TRIO * ((block - 1) // 3) + PIECE * ((block - 1) % 3)


def row_of(block, cut):
    return PIECE * cut if block == 0 else base_of(block) + TRIO * cut


def pick(choice, values):
    out = values[-1]
    for i in reversed(range(len(values) - 1)):
        out = jnp.where(choice == i, values[i], out)
    return out


def products(unit, at, right_hi, right_lo, left_hi, left_lo):
    k = pl.ds(256 * unit if isinstance(unit, int) else pl.multiple_of(256 * unit, 256), 256)

    def product(a, b):
        return lax.dot_general(a[k, :], b[k, at], (((0,), (0,)), ((), ())), preferred_element_type=jnp.float32)

    return product(left_hi, right_hi) + product(left_hi, right_lo) + product(left_lo, right_hi)


def last_unit(total, right_hi, right_lo, left_hi, left_lo, gram_ref, done, out_sem):
    def writing(n):
        at = pl.ds(n * WIDE if isinstance(n, int) else pl.multiple_of(n * WIDE, WIDE), WIDE)
        return pltpu.make_async_copy(done.at[n], gram_ref.at[:, at], out_sem.at[n])

    k = pl.ds(256 * 7, 256)
    high, low = left_hi[k, :].T, left_lo[k, :].T
    for n in range(SIDE // WIDE):
        at = pl.ds(n * WIDE, WIDE)

        def product(a, b):
            return jnp.dot(a, b[k, at], preferred_element_type=jnp.float32)

        done[n] = total[:, at] + product(high, right_hi) + product(high, right_lo) + product(low, right_hi)
        writing(n).start()

    for n in range(SIDE // WIDE):
        writing(n).wait()


def kernel(
    map_ref, weights_ref, mask_ref, total, right_hi, right_lo, left_hi, left_lo,
    store, relay, weights, mask, scales, columns,
    small_sem, load_sem, slot_sem, left_sem, relay_sem, scale_sem,
    sent_sem, sent_scale_sem, plus_sem, minus_sem, twin_sem, cross_sem, toward_sem, onward_sem,
):
    row, col = lax.axis_index("row"), lax.axis_index("col")
    x_lo, z = row // 8, row % 8
    x_hi, y, core = col // 8, (col // 2) % 4, col % 2
    up = (x_lo * 8 + (z + 1) % 8, col)
    down = (x_lo * 8 + (z + 7) % 8, col)
    pair = ((1 - x_lo) * 8 + z, col)
    twin = (row, x_hi * 8 + y * 2 + (1 - core))
    plus_0, plus = ((row, x_hi * 8 + ((y + 1) % 4) * 2 + n) for n in range(2))
    minus_0, minus = ((row, x_hi * 8 + ((y + 3) % 4) * 2 + n) for n in range(2))
    across_0, across = (((1 - x_lo) * 8 + z, (1 - x_hi) * 8 + y * 2 + n) for n in range(2))
    links = (up, down, pair)
    outer = x_hi == x_lo
    inner = x_hi != x_lo
    dy = (y + 4 - z // 2) % 4
    owner = (dy == 0) & (core == z % 2)
    first = jnp.where(outer & (dy == 0), core == z % 2, core == 1)

    def loading(cut):
        rows = pl.ds(PIECE * cut, PIECE)
        return pltpu.make_async_copy(map_ref.at[rows], store.at[rows], load_sem.at[cut])

    for cut in range(CUTS):
        loading(cut).start()
    small = (
        pltpu.make_async_copy(weights_ref, weights, small_sem.at[0]),
        pltpu.make_async_copy(mask_ref, mask, small_sem.at[1]),
    )
    for one in small:
        one.start()

    barrier = pltpu.get_barrier_semaphore()
    for other in (up, down, pair, twin, plus_0, plus, minus_0, minus, across_0, across):
        pl.semaphore_signal(barrier, inc=1, device_id=other, device_id_type=MESH)
    for one in small:
        one.wait()
    scales[pl.ds(0, 8), :] = jnp.broadcast_to(weights[...] * mask[...].astype(jnp.float32), (8, 128))
    pl.semaphore_wait(barrier, 10)

    def remote(source, target, sent, arrived, device):
        return pltpu.make_async_remote_copy(
            src_ref=source, dst_ref=target, send_sem=sent, recv_sem=arrived,
            device_id=device, device_id_type=MESH,
        )

    def arrival(ref, sem):
        return remote(ref, ref, sent_sem.at[0], sem, up)

    def span(start, size):
        return store.at[pl.ds(pl.multiple_of(start, 8), size)]

    def send_scale(source_block, step, g):
        remote(
            scales.at[pl.ds(8 * source_block, 8)],
            scales.at[pl.ds(pl.multiple_of(8 * (3 * step + 1 + g), 8), 8)],
            sent_scale_sem.at[0], scale_sem.at[step], links[g],
        ).start()

    for cut in range(CUTS):
        loading(cut).wait()
        if cut == 1:
            for g in range(3):
                send_scale(0, 0, g)
        for g in range(3):
            remote(
                span(PIECE * cut, PIECE), span(128 + TRIO * cut + PIECE * g, PIECE),
                sent_sem.at[0], slot_sem.at[cut], links[g],
            ).start()

    total[...] = jnp.zeros_like(total)

    def expand(block, start):
        square = jnp.broadcast_to(scales[pl.ds(pl.multiple_of(start, 8), 1), :], (128, 128))
        columns[block] = square.T

    back = (4 - dy) % 4
    hops = []
    for lane in range(4):
        on_outer = dy if lane % 2 == 0 else back
        on_inner = (1 + dy, 1 + back, pick(dy, (3, 2, 3, 4)), pick(dy, (3, 4, 3, 2)))[lane]
        hops.append(jnp.where(outer, on_outer, on_inner))
    late = [pick(hop, BEHIND) + jnp.where(first, 0, 1) for hop in hops]
    goes_plus = (
        jnp.where(outer, dy <= 2, dy <= 2),
        inner & (dy < 0),
        jnp.where(outer, dy <= 2, (dy == 1) | (dy == 2)),
        inner & (dy == 3),
    )
    goes_minus = (
        inner & (dy < 0),
        jnp.where(outer, dy != 1, dy != 1),
        inner & (dy == 1),
        jnp.where(outer, dy != 1, (dy == 2) | (dy == 3)),
    )
    at_source = outer & owner
    late_hops = jnp.where(outer, pick(dy, (0, 1, 2, 1)), pick(dy, (1, 2, 3, 2)))
    late_by = pick(late_hops, BEHIND) + jnp.where(first, 0, 1)
    ends = first & (dy == 0)
    late_plus = (first & (dy <= 1), ends)
    late_minus = (ends, first & ((dy == 0) | (dy == 3)))
    from_row = jnp.where(at_source, 0, LEFT)
    waits = jnp.logical_not(at_source)
    relays = inner & first & ((dy == 1) | (dy == 3))
    crosses = inner & owner
    sends_plus = [first & one for one in goes_plus]
    sends_minus = [first & one for one in goes_minus]

    def piece_of(slot, lane):
        third = (slot + 40 + lane) & 3
        there = (slot >= 0) & (slot < SLOTS) & ((third < 3) | (slot < CUTS))
        return jnp.where(third == 3, PIECE * slot, 128 + TRIO * slot + PIECE * third), there

    def pass_on(slot, lane, at, source_row, device, sent):
        remote(span(source_row + at, PIECE), span(LEFT + at, PIECE), sent, left_sem.at[lane, slot], device).start()

    def held(slot):
        return relay.at[pl.ds(pl.multiple_of(PIECE * slot, 8), PIECE)]

    def into_relay(slot, at, device, sent):
        remote(span(at, PIECE), held(slot), sent, relay_sem.at[slot], device).start()

    def out_of_relay(slot, lane, at):
        arrival(held(slot), relay_sem.at[slot]).wait_recv()
        remote(held(slot), span(LEFT + at, PIECE), onward_sem.at[0], left_sem.at[lane, slot], across).start()

    def split(turn, start, phase, base, pieces, first_cut=0, end_cut=CUTS):
        cut = turn - start

        @pl.when((turn >= start + first_cut) & (turn < start + end_cut))
        def _():
            for n in range(pieces):
                (right_o, left_o), (right_i, left_i) = OUTER[phase][n], INNER[phase][n]

                def start_of(a, b):
                    def one(block):
                        return PIECE * cut if block == 0 else base_of(block) + TRIO * cut

                    return one(a) if a == b else jnp.where(outer, one(a), one(b))

                right_row = pl.multiple_of(start_of(right_o, right_i), 8)
                left_row = pl.multiple_of(LEFT + start_of(left_o, left_i), 8)
                block = right_o if right_o == right_i else jnp.where(outer, right_o, right_i)
                put = pl.ds(pl.multiple_of(base + PIECE * (pieces * cut + n), 16), PIECE)
                factor = columns[block, pl.ds(pl.multiple_of(PIECE * cut, 8), PIECE), :]
                for lane in range(SIDE // 128):
                    at = pl.ds(128 * lane, 128)
                    value = store[pl.ds(right_row, PIECE), at] * factor
                    high = value.astype(jnp.bfloat16)
                    right_hi[put, at] = high
                    right_lo[put, at] = (value - high.astype(jnp.float32)).astype(jnp.bfloat16)
                left_from = jnp.where(at_source, left_row - LEFT, left_row)
                value = store[pl.ds(pl.multiple_of(left_from, 8), PIECE), :]
                high = value.astype(jnp.bfloat16)
                left_hi[put, :] = high
                left_lo[put, :] = (value - high.astype(jnp.float32)).astype(jnp.bfloat16)

    def multiply(unit, n):
        at = pl.ds(pl.multiple_of(256 * n, 256), 256)
        total[:, at] += products(unit, at, right_hi, right_lo, left_hi, left_lo)

    def gathering(turn):
        step, cut = turn >> 3, turn & 7
        arrival(span(128 + TRIO * turn, TRIO), slot_sem.at[turn]).wait_recv()

        @pl.when(cut == 0)
        def _():
            arrival(scales.at[pl.ds(pl.multiple_of(8 + 24 * step, 8), 24)], scale_sem.at[step]).wait_recv()
            for g in range(3):
                @pl.when(step < STEPS - 1)
                def _():
                    source = pick(step, tuple(PARENT[s][g] for s in range(1, STEPS)))
                    remote(
                        scales.at[pl.ds(pl.multiple_of(8 * source, 8), 8)],
                        scales.at[pl.ds(pl.multiple_of(8 * (3 * step + 4 + g), 8), 8)],
                        sent_scale_sem.at[0], scale_sem.at[step + 1], links[g],
                    ).start()

        @pl.when(step < STEPS - 1)
        def _():
            for g in range(3):
                base = pick(step, tuple(base_of(PARENT[s][g]) for s in range(1, STEPS)))
                remote(
                    span(base + TRIO * cut, PIECE), span(128 + TRIO * (turn + CUTS) + PIECE * g, PIECE),
                    sent_sem.at[step + 1], slot_sem.at[turn + CUTS], links[g],
                ).start()

        @pl.when(crosses)
        def _():
            for lane in range(4):
                at, there = piece_of(turn, lane)

                @pl.when(there)
                def _():
                    @pl.when(turn >= LATE)
                    def _():
                        pass_on(turn, lane, at, 0, across, cross_sem.at[1])

                    @pl.when(turn < LATE)
                    def _():
                        if lane < 2:
                            pass_on(turn, lane, at, 0, across, cross_sem.at[0])
                        else:
                            into_relay(turn, at, (plus, minus)[lane - 2], toward_sem.at[lane - 2])

    def rest_of(turn, first_turn, end_turn):
        @pl.when(relays)
        def _():
            slot = turn - BEHIND[1]
            for lane, place in ((2, 1), (3, 3)):
                at, there = piece_of(slot, lane)

                @pl.when((dy == place) & there & (slot < LATE))
                def _():
                    out_of_relay(slot, lane, at)

        def forward(slot, lane, at, on_plus, on_minus, sems):
            @pl.when(waits)
            def _():
                arrival(span(LEFT + at, PIECE), left_sem.at[lane, slot]).wait_recv()

            @pl.when(on_plus)
            def _():
                pass_on(slot, lane, at, from_row, plus, plus_sem.at[sems + lane])

            @pl.when(on_minus)
            def _():
                pass_on(slot, lane, at, from_row, minus, minus_sem.at[sems + lane])

            @pl.when(first)
            def _():
                pass_on(slot, lane, at, from_row, twin, twin_sem.at[lane])

        is_late = (turn - late_by >= LATE) & (turn - late_by < SLOTS)

        @pl.when(is_late)
        def _():
            slot = turn - late_by
            for lane in range(4):
                at, there = piece_of(slot, lane)

                @pl.when(there)
                def _():
                    forward(slot, lane, at, late_plus[lane % 2], late_minus[lane % 2], 4)

        for lane in range(4):
            slot = turn - late[lane]
            at, there = piece_of(slot, lane)

            @pl.when(there & (slot < LATE))
            def _():
                forward(slot, lane, at, sends_plus[lane], sends_minus[lane], 0)

        for phase, blocks in ((0, range(7)), (1, range(7, 10)), (2, range(10, 13)), (3, range(13, 16))):
            if first_turn <= STARTS[phase] < end_turn:
                @pl.when(turn == STARTS[phase])
                def _():
                    for block in blocks:
                        expand(block, 8 * block)

        late_cut = LATE % CUTS
        for phase, sooner, first_cut, end_cut in (
            (0, 0, 0, CUTS), (1, 0, 0, CUTS), (2, 0, 0, CUTS), (3, 0, 0, CUTS),
            (4, 0, 0, late_cut), (4, SOONER, late_cut, CUTS),
        ):
            start = STARTS[phase] - sooner
            if start + first_cut < end_turn and start + end_cut > first_turn:
                split(turn, start, phase, FIRST_ROWS[phase], len(OUTER[phase]), first_cut, end_cut)

        dots_here = [one for n, one in enumerate(DOTS) if one[0] < end_turn and (n + 1 == len(DOTS) or DOTS[n + 1][0] > first_turn)]
        begun, unit, ahead, pace = dots_here[0]
        for one in dots_here[1:]:
            begun, unit, ahead, pace = (jnp.where(turn >= one[0], new, old) for new, old in zip(one, (begun, unit, ahead, pace)))
        quarter = ahead + pace * (turn - begun)

        @pl.when((quarter >= 0) & (quarter < 4))
        def _():
            @pl.loop(quarter, quarter + pace)
            def _(n):
                multiply(unit, n)

    @pl.loop(0, SLOTS)
    def _(turn):
        gathering(turn)
        rest_of(turn, 0, SLOTS)

    @pl.loop(SLOTS, TURNS)
    def _(turn):
        rest_of(turn, SLOTS, TURNS)

    for step in range(STEPS):
        remote(
            span(0, CUTS * TRIO), span(0, CUTS * TRIO), sent_sem.at[step], slot_sem.at[0], up
        ).wait_send()
    remote(
        scales.at[pl.ds(8, 120)], scales.at[pl.ds(8, 120)], sent_scale_sem.at[0], slot_sem.at[0], up
    ).wait_send()

    def drain(sem, rows):
        remote(span(0, rows), span(0, rows), sem, slot_sem.at[0], up).wait_send()

    for lane in range(4):
        soon, later = rows_of(lane, 0, LATE), rows_of(lane, LATE, SLOTS)
        for condition, sem, rows in (
            (sends_plus[lane], plus_sem.at[lane], soon),
            (sends_minus[lane], minus_sem.at[lane], soon),
            (late_plus[lane % 2], plus_sem.at[4 + lane], later),
            (late_minus[lane % 2], minus_sem.at[4 + lane], later),
            (first, twin_sem.at[lane], soon + later),
        ):
            @pl.when(condition)
            def _():
                drain(sem, rows)

    @pl.when(crosses)
    def _():
        drain(cross_sem.at[0], rows_of(0, 0, LATE) + rows_of(1, 0, LATE))
        drain(cross_sem.at[1], sum(rows_of(lane, LATE, SLOTS) for lane in range(4)))
        drain(toward_sem.at[0], rows_of(2, 0, LATE))
        drain(toward_sem.at[1], rows_of(3, 0, LATE))

    for lane, place in ((2, 1), (3, 3)):
        @pl.when(relays & (dy == place))
        def _():
            drain(onward_sem.at[0], rows_of(lane, 0, LATE))


def per_device(forward_map, sensor_weights, sensor_mask):
    dma = pltpu.SemaphoreType.DMA
    half = pltpu.VMEM((OBS, SIDE), jnp.bfloat16)
    parts = pl.pallas_call(
        kernel,
        out_shape=(pltpu.VMEM((SIDE, SIDE), jnp.float32), half, half, half, half),
        in_specs=[
            pl.BlockSpec(memory_space=pltpu.HBM),
            pl.BlockSpec(memory_space=pltpu.HBM),
            pl.BlockSpec(memory_space=pltpu.HBM),
        ],
        out_specs=(pl.BlockSpec(memory_space=pltpu.VMEM),) * 5,
        scratch_shapes=[
            pltpu.VMEM((2 * OBS, SIDE), jnp.float32),
            pltpu.VMEM((PIECE * SLOTS, SIDE), jnp.float32),
            pltpu.VMEM((1, 128), jnp.float32),
            pltpu.VMEM((1, 128), jnp.int32),
            pltpu.VMEM((128, 128), jnp.float32),
            pltpu.VMEM((16, 128, 128), jnp.float32),
            dma((2,)), dma((CUTS,)), dma((SLOTS,)), dma((4, SLOTS)), dma((SLOTS,)), dma((STEPS,)),
            dma((STEPS,)), dma((1,)), dma((8,)), dma((8,)), dma((4,)), dma((2,)), dma((2,)), dma((1,)),
        ],
        compiler_params=pltpu.CompilerParams(
            collective_id=0, has_side_effects=True, vmem_limit_bytes=67043328 - 20 * SIDE * SIDE
        ),
        cost_estimate=pl.CostEstimate(
            flops=2 * OBS * SIDE * SIDE, bytes_accessed=8 * SIDE * SIDE, transcendentals=0
        ),
    )(forward_map, sensor_weights.reshape(1, -1), sensor_mask.reshape(1, -1))
    return pl.pallas_call(
        last_unit,
        out_shape=jax.ShapeDtypeStruct((SIDE, SIDE), jnp.float32),
        in_specs=[pl.BlockSpec(memory_space=pltpu.VMEM)] * 5,
        out_specs=pl.BlockSpec(memory_space=pl.ANY),
        scratch_shapes=[pltpu.VMEM((SIDE // WIDE, SIDE, WIDE), jnp.float32), dma((SIDE // WIDE,))],
        compiler_params=pltpu.CompilerParams(vmem_limit_bytes=16 * 1024 * 1024),
        cost_estimate=pl.CostEstimate(flops=2 * 256 * SIDE * SIDE, bytes_accessed=4 * SIDE * SIDE, transcendentals=0),
    )(*parts)


def solution(mesh):
    placed = (P("row", "col"), P("row"), P("row"))
    return jax.shard_map(
        per_device, mesh=mesh, in_specs=placed, out_specs=P("row", "col"), check_vma=False
    )
```
